128 devices in a mesh: seq: 32 (over y, x, z_lo), head: 4 (over z_hi, core).
Axes of the slice: x: 4, y: 4, z: 4 (z_hi: 2, z_lo: 2; z = z_hi * 2 + z_lo), core: 2. Of those that a mesh axis runs over, the one named last changes fastest.
Arguments:
- tokens: bfloat16 [32, 4096, 1024], P('seq'), may hold values from -6 to 6
- w_query: bfloat16 [1024, 1024], P(None, 'head'), may hold values from -1 to 1
- w_key: bfloat16 [1024, 1024], P(None, 'head'), may hold values from -1 to 1
- w_value: bfloat16 [1024, 1024], P(None, 'head'), may hold values from -0.1875 to 0.1875
- w_out: bfloat16 [1024, 1024], P('head'), may hold values from -0.1875 to 0.1875
Outputs:
- mixed: bfloat16 [32, 4096, 1024], P('seq', None, 'head')
The draws below stay inside these ranges and needn't reach their ends.
All inputs are finite; a program needn't handle non-finite values.
Results may differ from the reference program's by a relative error of at most 0.012.
Values may be sent and summed in bfloat16 or wider, within the bound.
A program may use at most 128 MiB of HBM per device.

```python
import jax
import jax.numpy as jnp
from jax import lax

D = 1024
HEADS = 16
FRAMES = 32
PATCHES = 4096


def query_key_pair(key):
    shape_full = (D, D)
    base = jnp.clip(jax.random.normal(jax.random.fold_in(key, 11), shape_full, jnp.float32), -6.0, 6.0)
    other = jnp.clip(jax.random.normal(jax.random.fold_in(key, 12), shape_full, jnp.float32), -6.0, 6.0)
    return (base * D ** (-0.5), other * D ** (-0.5))


def draw_w_query(key, part):
    first, second = query_key_pair(key)
    return first.astype(jnp.bfloat16)


def draw_w_key(key, part):
    first, second = query_key_pair(key)
    return second.astype(jnp.bfloat16)


def steps_of(own_key, extent, shards, low, high):
    level = 1.0
    for dim, parts in shards:
        draws = jax.random.uniform(jax.random.fold_in(jax.random.fold_in(own_key, 6), dim), (parts,), jnp.float32, low / len(shards), high / len(shards))
        level = level * jnp.repeat(jnp.exp(draws), extent[dim] // parts).reshape((-1,) + (1,) * (len(extent) - 1 - dim))
    return level


def noise(rng, extent, spread, limit, split=(), dtype=jnp.bfloat16):
    array = spread * jax.random.normal(rng, extent, jnp.float32)
    if split:
        array = array * steps_of(rng, extent, split, -0.22, 0.18)
    return jnp.clip(array, -limit, limit).astype(dtype)


def setup_inputs(seed: int = 0) -> dict:
    streams_of = jax.random.split(jax.random.key(seed), 6)
    tokens = noise(streams_of[0], (FRAMES, PATCHES, D), 1.0, 6.0, ((0, 32),))
    w_query = draw_w_query(jax.random.fold_in(streams_of[5], 71), 0)
    w_key = draw_w_key(jax.random.fold_in(streams_of[5], 71), 0)
    w_value = noise(streams_of[3], (D, D), D ** -0.5, 0.1875, ((1, 4),))
    w_out = noise(streams_of[4], (D, D), D ** -0.5, 0.1875, ((0, 4),))
    return {"tokens": tokens, "w_query": w_query, "w_key": w_key, "w_value": w_value, "w_out": w_out}


epsilon = 1e-05

def normalize(tokens):
    values = tokens.astype(jnp.float32)
    row_mean = lax.optimization_barrier(jnp.mean(values, axis=-1, keepdims=True))
    centered = values - row_mean
    row_var = lax.optimization_barrier(jnp.mean(centered * centered, axis=-1, keepdims=True))
    return (centered * lax.rsqrt(row_var + epsilon)).astype(jnp.bfloat16)

def project(source, weight):
    frames, patch_count, width = source.shape
    flat = jnp.dot(source.reshape(frames * patch_count, width), weight, preferred_element_type=jnp.float32)
    return flat.astype(jnp.bfloat16).reshape(frames, patch_count, weight.shape[1])

def attend(queries, key_rows, value_rows, head_count):
    frames, patch_count, feature_width = queries.shape
    head_size = feature_width // head_count
    query_flat = queries.reshape(frames, patch_count * head_count, head_size).astype(jnp.float32)
    key_flat = key_rows.reshape(frames, patch_count * head_count, head_size).astype(jnp.float32)
    value_flat = value_rows.reshape(frames, patch_count * head_count, head_size).astype(jnp.float32)
    scores = jnp.einsum('fmd,gmd->fgm', query_flat, key_flat) * head_size ** (-0.5)
    row_top = lax.optimization_barrier(jnp.max(scores, axis=1, keepdims=True))
    raised = jnp.exp(scores - row_top)
    weights = (raised / lax.optimization_barrier(jnp.sum(raised, axis=1, keepdims=True))).astype(jnp.bfloat16)
    attended = jnp.einsum('fgm,gmd->fmd', weights.astype(jnp.float32), value_flat)
    return attended.astype(jnp.bfloat16).reshape(frames, patch_count, feature_width)

def reference(tokens, w_query, w_key, w_value, w_out):
    normed = normalize(tokens)
    queries = project(normed, w_query)
    key_rows = project(normed, w_key)
    value_rows = project(normed, w_value)
    attended = attend(queries, key_rows, value_rows, HEADS)
    return project(attended, w_out)
```

```python
import jax
import jax.numpy as jnp
from jax import lax
from jax.experimental import pallas as pl
from jax.experimental.pallas import tpu as pltpu
from jax.sharding import PartitionSpec as P

MESH = pl.DeviceIdType.MESH
EPS = 1e-5
LOG2E = 1.4426950408889634
HS = 64
CHUNKS = 4
BF = jnp.bfloat16
F32 = jnp.float32


def remote(src, dst, send, recv, seq, head):
    return pltpu.make_async_remote_copy(
        src_ref=src,
        dst_ref=dst,
        send_sem=send,
        recv_sem=recv,
        device_id=(seq, head),
        device_id_type=MESH,
    )


def wait_bytes(ref, sem):
    pltpu.make_async_copy(ref, ref, sem).wait()


def kernel(
    tok, wq, wk, wv, wo, out,
    xb, xn, wqb, wkb, wvb, wob, att, ob,
    local_sem, own_sem, tok_send, tok_recv, cross_send, cross_recv, next_send, next_recv,
    sib_send, sib_recv, out_send, out_recv, ready,
):
    s, h = lax.axis_index("seq"), lax.axis_index("head")
    y, x, zl = s // 8, (s // 2) % 4, s % 2
    zh, core = h // 2, h % 2
    z = zh * 2 + zl
    block = h * 32 + s
    sib = zh * 2 + (1 - core)
    over = (1 - zh) * 2 + core
    over_sib = (1 - zh) * 2 + (1 - core)
    weights = ((wq, wqb, 1024, 128), (wk, wkb, 1024, 128), (wv, wvb, 1024, 128), (wo, wob, 256, 32))

    for hbm, buf, depth, _ in weights:
        pltpu.make_async_copy(hbm, buf.at[pl.ds(h * depth, depth)], local_sem).start()
    own = pltpu.make_async_copy(tok.at[pl.ds(block * CHUNKS, CHUNKS)], xb.at[:, s], own_sem)
    own.start()

    barrier = pltpu.get_barrier_semaphore()

    def greet(i, carry):
        pl.semaphore_signal(barrier, inc=1, device_id=(lax.rem(s + i, 32), h), device_id_type=MESH)
        return carry

    across = (y * 8 + x * 2 + (1 - zl), over)
    pl.semaphore_signal(barrier, inc=1, device_id=across, device_id_type=MESH)
    for i in range(1, 4):
        pl.semaphore_signal(barrier, inc=1, device_id=(s, lax.rem(h + i, 4)), device_id_type=MESH)
    lax.fori_loop(1, 32, greet, 0)
    pl.semaphore_wait(barrier, 35)
    for i in range(1, 4):
        pl.semaphore_signal(ready, inc=1, device_id=(s, lax.rem(h + i, 4)), device_id_type=MESH)

    def piece(buf, shard, depth, rows, i):
        return buf.at[pl.ds(pl.multiple_of(shard * depth + i * rows, rows), rows)]

    for r in range(2):
        for i in (lax.rem(x + 2 * r, 4), 4 + lax.rem(y + 2 * r, 4)):
            for hbm, buf, depth, rows in weights:
                remote(
                    piece(hbm, 0, depth, rows, i), piece(buf, h, depth, rows, i),
                    cross_send, cross_recv.at[r], *across,
                ).start()
    for hbm, buf, depth, _ in weights:
        remote(hbm, buf.at[pl.ds(h * depth, depth)], sib_send.at[0], sib_recv.at[0], s, sib).start()

    def send_tokens(chunk):
        def one(o, carry):
            dx, dy, dz = o % 4, (o // 4 + o) % 4, (o // 16 + o // 2) % 2
            t = ((y + dy) % 4) * 8 + ((x + dx) % 4) * 2 + (zl + dz) % 2

            @pl.when(o > 0)
            def _():
                remote(
                    tok.at[(h * 32 + t) * CHUNKS + chunk], xb.at[chunk, s],
                    tok_send, tok_recv.at[chunk], t, h,
                ).start()

            return carry

        lax.fori_loop(0, 32, one, 0)

    def normalize(chunk):
        wait_bytes(xb.at[chunk, pl.ds(0, 31)], tok_recv.at[chunk])

        def rows(b, carry):
            t = xb[chunk, pl.ds(b * 8, 8)].astype(F32)
            centered = t - jnp.mean(t, axis=-1, keepdims=True)
            var = jnp.mean(centered * centered, axis=-1, keepdims=True)
            n = (centered * lax.rsqrt(var + EPS)).reshape(64, 1024)
            xn[chunk, pl.ds(pl.multiple_of(b * 64, 64), 64), :] = n.astype(BF)
            return carry

        lax.fori_loop(0, 4, rows, 0)

    def send_out(pair):
        def one(o, carry):
            dc, p = o // 64, o % 64
            dx, dy, dz = p % 4, (p // 4 + p) % 4, (p // 16 + p) % 4
            zz, cc = (z + dz) % 4, (core + dc) % 2
            t = ((y + dy) % 4) * 8 + ((x + dx) % 4) * 2 + zz % 2
            th = (zz // 2) * 2 + cc

            @pl.when(o > 0)
            def _():
                remote(
                    ob.at[t, pl.ds(pair * 2, 2), :, pl.ds(pl.multiple_of(th * 256, 256), 256)],
                    out.at[pl.ds(block * CHUNKS + pair * 2, 2)],
                    out_send, out_recv, t, th,
                ).start()

            return carry

        lax.fori_loop(0, 128, one, 0)
        pltpu.make_async_copy(
            ob.at[s, pl.ds(pair * 2, 2), :, pl.ds(pl.multiple_of(h * 256, 256), 256)],
            out.at[pl.ds(block * CHUNKS + pair * 2, 2)],
            own_sem,
        ).start()

    def project_out(chunk):
        def columns(n, carry):
            cols = pl.ds(pl.multiple_of(n * 256, 256), 256)
            m = jnp.dot(att[chunk], wob[:, cols], preferred_element_type=F32)
            ob[:, chunk, :, cols] = m.reshape(32, 8, 256).astype(BF)
            return carry

        lax.fori_loop(0, 4, columns, 0)

    row_patch = lax.broadcasted_iota(jnp.int32, (8, 256), 0)
    lane_patch = lax.broadcasted_iota(jnp.int32, (8, 256), 1) % 8
    same_patch = row_patch == lane_patch

    def attend(chunk, shard):
        rows = pl.ds(pl.multiple_of(shard * 1024, 1024), 1024)
        xc = xn[chunk]
        q = jnp.dot(xc, wqb[rows, :], preferred_element_type=F32) * (LOG2E * HS**-0.5)
        k = jnp.dot(xc, wkb[rows, :], preferred_element_type=F32).astype(BF)
        v = jnp.dot(xc, wvb[rows, :], preferred_element_type=F32)
        qt = q.T.astype(BF)
        vt = v.T.astype(BF)
        nothing = jnp.zeros((HS, 256), BF)
        parts = []
        for j in range(4):
            mine = qt[j * HS : (j + 1) * HS]
            padded = jnp.concatenate([mine, nothing] if j % 2 == 0 else [nothing, mine], axis=0)
            pair = k[:, (j // 2) * 128 : (j // 2) * 128 + 128]
            score = jnp.dot(pair, padded, preferred_element_type=F32).reshape(32, 8, 256)
            top = jnp.where(same_patch, jnp.max(score, axis=0), 3e38)
            raised = jnp.exp2(score - top[None])
            total = jnp.sum(jnp.sum(raised, axis=0), axis=0, keepdims=True)
            weight = raised.reshape(256, 256).astype(BF)
            got = jnp.dot(vt[j * HS : (j + 1) * HS], weight, preferred_element_type=F32)
            parts.append(got / total)
        cols = pl.ds(pl.multiple_of(shard * 256, 256), 256)
        att[chunk, :, cols] = jnp.concatenate(parts, axis=0).T.astype(BF)

    send_tokens(0)
    send_tokens(1)
    wait_bytes(wqb, local_sem)
    own.wait()

    def step(i, carry):
        @pl.when(i == 0)
        def _():
            normalize(0)
            wait_bytes(wqb, sib_recv.at[0])

        @pl.when(i == 2)
        def _():
            wait_bytes(wqb.at[pl.ds(0, 1024)], cross_recv.at[0])
            for _, buf, depth, rows in weights:
                at = piece(buf, over, depth, rows, x)
                for d in (1, 3):
                    t = y * 8 + lax.rem(x + d, 4) * 2 + zl
                    remote(at, at, next_send, next_recv, t, h).start()
                up = piece(buf, over, depth, rows, 4 + y)
                for d in (1, 3):
                    t = lax.rem(y + d, 4) * 8 + x * 2 + zl
                    remote(up, up, next_send, next_recv, t, h).start()
                remote(at, at, sib_send.at[1], sib_recv.at[1], s, sib).start()
                remote(up, up, sib_send.at[1], sib_recv.at[1], s, sib).start()
            send_tokens(2)
            send_tokens(3)
            normalize(1)

        @pl.when(i == 4)
        def _():
            wait_bytes(wqb.at[pl.ds(0, 1024)], cross_recv.at[1])
            for _, buf, depth, rows in weights:
                for p in (lax.rem(x + 2, 4), 4 + lax.rem(y + 2, 4)):
                    at = piece(buf, over, depth, rows, p)
                    remote(at, at, sib_send.at[1], sib_recv.at[1], s, sib).start()
            normalize(2)

        @pl.when(i == 6)
        def _():
            wait_bytes(wqb.at[pl.ds(0, 2048)], next_recv)
            for _, buf, depth, rows in weights:
                for d in (1, 3):
                    for p in (lax.rem(x + d, 4), 4 + lax.rem(y + d, 4)):
                        at = piece(buf, over, depth, rows, p)
                        remote(at, at, sib_send.at[1], sib_recv.at[1], s, sib).start()
            wait_bytes(wqb, sib_recv.at[1])

        @pl.when(i == 10)
        def _():
            lax.fori_loop(0, 2, lambda n, carry: (project_out(n), carry)[1], 0)
            pl.semaphore_wait(ready, 3)
            send_out(0)

        @pl.when(i == 12)
        def _():
            normalize(3)

        g = i // 2
        late = g >= 6
        chunk = jnp.where(late, 3, g % 3)
        away = jnp.where(late, g - 6, g // 3)
        half = jnp.where(away == 0, zh, 1 - zh)
        attend(chunk, half * 2 + i % 2)
        return carry

    lax.fori_loop(0, 16, step, 0)
    lax.fori_loop(2, 4, lambda n, carry: (project_out(n), carry)[1], 0)
    send_out(1)

    wait_bytes(out.at[pl.ds(0, 127 * CHUNKS)], out_recv)
    wait_bytes(out.at[pl.ds(0, CHUNKS)], own_sem)
    wait_bytes(out.at[pl.ds(0, 127 * CHUNKS)], out_send)
    wait_bytes(xb.at[:, pl.ds(0, 31)], tok_send)
    wait_bytes(wqb.at[pl.ds(0, 2048)], cross_send)
    wait_bytes(wqb.at[pl.ds(0, 2048)], next_send)
    wait_bytes(wqb, sib_send.at[0])
    wait_bytes(wqb, sib_send.at[1])


def local(tokens, w_query, w_key, w_value, w_out):
    hbm = pl.BlockSpec(memory_space=pltpu.HBM)
    dma = pltpu.SemaphoreType.DMA
    mixed = pl.pallas_call(
        kernel,
        out_shape=jax.ShapeDtypeStruct((512, 8, 256), BF),
        in_specs=[hbm] * 5,
        out_specs=pl.BlockSpec(memory_space=pl.ANY),
        scratch_shapes=[
            pltpu.VMEM((CHUNKS, 32, 8, 1024), BF),
            pltpu.VMEM((CHUNKS, 256, 1024), BF),
            pltpu.VMEM((4096, 256), BF),
            pltpu.VMEM((4096, 256), BF),
            pltpu.VMEM((4096, 256), BF),
            pltpu.VMEM((1024, 1024), BF),
            pltpu.VMEM((CHUNKS, 256, 1024), BF),
            pltpu.VMEM((32, CHUNKS, 8, 1024), BF),
            dma,
            dma,
            dma,
            dma((CHUNKS,)),
            dma,
            dma((2,)),
            dma,
            dma,
            dma((2,)),
            dma((2,)),
            dma,
            dma,
            pltpu.SemaphoreType.REGULAR,
        ],
        compiler_params=pltpu.CompilerParams(
            collective_id=0, has_side_effects=True, vmem_limit_bytes=32 * 2**20
        ),
        name="temporal",
    )(tokens.reshape(512, 8, 1024), w_query, w_key, w_value, w_out)
    return mixed.reshape(1, 4096, 256)


def solution(mesh):
    return jax.shard_map(
        local,
        mesh=mesh,
        in_specs=(
            P("seq", None, None),
            P(None, "head"),
            P(None, "head"),
            P(None, "head"),
            P("head", None),
        ),
        out_specs=P("seq", None, "head"),
        check_vma=False,
    )
```
